32 devices in a mesh: expert: 8 (over z, x), shard: 4 (over y, core).
Axes of the slice: x: 2, y: 2, z: 4, core: 2. Of those that a mesh axis runs over, the one named last changes fastest.
Arguments:
- master_down: float32 [128, 768, 2048], P('expert', None, 'shard'), may hold values from -0.3125 to 0.3125
- router_weight: float32 [2048, 128], P('shard', 'expert'), may hold values from -0.125 to 0.125
- router_gain: float32 [2048], P('shard'), may hold values from 0.25 to 1.75
Outputs:
- final_down: bfloat16 [128, 768, 2048], P('expert')
- scale_down: float32 [128, 768], P('expert')
- serve_router: bfloat16 [2048, 128], replicated
The draws below stay inside these ranges and needn't reach their ends.
All inputs are finite; a program needn't handle non-finite values.
Results may differ from the reference program's by a relative error of at most 0.001.
Values may be sent and summed in bfloat16 or wider, within the bound.
A program may use at most 192 MiB of HBM per device.

```python
import jax
import jax.numpy as jnp
from jax import lax

EXPERTS = 128
D_MODEL = 2048
D_EXPERT = 768


def strengthened(result, rng, source, target, blocks, factor):
    owner, partner = [(jnp.arange(result.shape[axis_at]) // (result.shape[axis_at] // blocks)).reshape([-1 if axis == axis_at else 1 for axis in range(result.ndim)]) for axis_at in (source, target)]
    chosen = jax.random.permutation(rng, blocks)[partner]
    strong = (owner == chosen) | (owner == (partner + blocks // 2) % blocks)
    return jnp.where(strong, factor * result, result)


def levels(key, extent, pieces, least, top_value):
    def one(dim, parts):
        steps = jax.random.uniform(jax.random.fold_in(jax.random.fold_in(key, 6), dim), (parts,), jnp.float32, least / len(pieces), top_value / len(pieces))
        return jnp.repeat(jnp.exp(steps), extent[dim] // parts).reshape((-1,) + (1,) * (len(extent) - dim - 1))

    factor_of = one(*pieces[0])
    for cut in pieces[1:]:
        factor_of = factor_of * one(*cut)
    return factor_of


def centred(rng, extent, spread, reach, cuts=(), held_as=jnp.bfloat16):
    drawn = jax.random.normal(rng, extent, jnp.float32) * spread
    if len(cuts) > 0:
        drawn = levels(rng, extent, cuts, -0.22, 0.18) * drawn
    return jnp.clip(drawn, min=-reach, max=reach).astype(held_as)


def bell_draw_with(rng, dims, deviation, most, pieces, heavy, held_as=jnp.bfloat16):
    drawn = deviation * jax.random.normal(rng, dims, jnp.float32)
    if pieces:
        drawn = drawn * levels(rng, dims, pieces, -0.22, 0.18)
    return jnp.clip(strengthened(drawn, jax.random.fold_in(rng, 3), *heavy), -most, most).astype(held_as)


def setup_inputs(seed: int = 0) -> dict:
    key_of = jax.random.split(jax.random.key(seed), 4)
    master_down = bell_draw_with(key_of[0], (EXPERTS, D_EXPERT, D_MODEL), D_EXPERT ** -0.5, 0.3125, ((0, 8), (2, 4)), (2, 1, 4, 2.0), jnp.float32)
    router_weight = centred(key_of[1], (D_MODEL, EXPERTS), D_MODEL ** -0.5, 0.125, ((0, 4), (1, 8)), jnp.float32)
    router_gain = jnp.clip(1.0 + 0.15 * jax.random.normal(key_of[2], (D_MODEL,), jnp.float32), 0.25, 1.75)
    return dict(master_down=master_down, router_weight=router_weight, router_gain=router_gain)


def reference(master_down, router_weight, router_gain):
    scale_down = jnp.sqrt(lax.optimization_barrier(jnp.sum(master_down * master_down, axis=2)))
    final_down = (master_down / jnp.expand_dims(scale_down, 2)).astype(jnp.bfloat16)
    serve_router = (router_weight * router_gain[:, None]).astype(jnp.bfloat16)
    return (final_down, scale_down, serve_router)
```

```python
import functools

import jax
import jax.numpy as jnp
from jax import lax
from jax.experimental import pallas as pl
from jax.experimental.pallas import tpu as pltpu
from jax.sharding import PartitionSpec as P


def sum_kernel(n, part_ref, scale_ref, slots, send_sem, recv_sem):
    me = lax.axis_index("shard")
    barrier = pltpu.get_barrier_semaphore()
    for step in range(1, n):
        pl.semaphore_signal(
            barrier,
            inc=1,
            device_id={"shard": lax.rem(me + step, n)},
            device_id_type=pl.DeviceIdType.MESH,
        )
    pl.semaphore_wait(barrier, n - 1)
    copies = []
    for step in range(1, n):
        copies.append(
            pltpu.make_async_remote_copy(
                src_ref=part_ref,
                dst_ref=slots.at[me],
                send_sem=send_sem.at[step - 1],
                recv_sem=recv_sem.at[step - 1],
                device_id={"shard": lax.rem(me + step, n)},
                device_id_type=pl.DeviceIdType.MESH,
            )
        )
        copies[-1].start()
    slots[me] = part_ref[...]
    for copy in copies:
        copy.wait()
    total = slots[0]
    for step in range(1, n):
        total = total + slots[step]
    scale_ref[...] = jnp.sqrt(total)


def summed_scale(part, n):
    return pl.pallas_call(
        functools.partial(sum_kernel, n),
        out_shape=jax.ShapeDtypeStruct(part.shape, jnp.float32),
        in_specs=[pl.BlockSpec(memory_space=pltpu.VMEM)],
        out_specs=pl.BlockSpec(memory_space=pltpu.VMEM),
        scratch_shapes=[
            pltpu.VMEM((n,) + part.shape, jnp.float32),
            pltpu.SemaphoreType.DMA((n - 1,)),
            pltpu.SemaphoreType.DMA((n - 1,)),
        ],
        compiler_params=pltpu.CompilerParams(collective_id=0, has_side_effects=True),
        name="sum_squares",
    )(part)


def place_kernel(offsets, *refs):
    me = lax.axis_index("shard")
    out_ref = refs[-1]
    for offset, ref in zip(offsets, refs):
        wide = ref.shape[1]
        at = pl.multiple_of(lax.bitwise_xor(me, jnp.int32(offset)) * wide, wide)
        out_ref[:, pl.ds(at, wide)] = ref[...]


def place(out, pieces, first, unit, rows):
    offsets = [offset for offset, _ in pieces]
    arrays = [array for _, array in pieces]
    tall, wide = arrays[0].shape
    in_specs = [pl.BlockSpec((unit, wide), lambda i: (i, 0))] * len(arrays)
    aliases = {}
    if out is not None:
        aliases = {len(arrays): 0}
        arrays.append(out)
        in_specs = in_specs + [pl.BlockSpec(memory_space=pl.ANY)]
    full = wide * len(offsets)
    return pl.pallas_call(
        functools.partial(place_kernel, offsets),
        grid=(tall // unit,),
        out_shape=jax.ShapeDtypeStruct((rows, full), jnp.bfloat16),
        in_specs=in_specs,
        out_specs=pl.BlockSpec((unit, full), lambda i: (first // unit + i, 0)),
        input_output_aliases=aliases,
        cost_estimate=pl.CostEstimate(
            flops=tall * full, bytes_accessed=4 * tall * full, transcendentals=0
        ),
        name="place",
    )(*arrays)


def chunks(rows, inner):
    unit = inner // 2
    left = rows // unit
    most = max(1, left // 8)
    first = 0
    while left:
        take = max(1, min(most, left // 2))
        yield first, take * unit, unit
        first += take * unit
        left -= take


def doubled(array, n):
    held = [(0, array)]
    bit = n // 2
    while bit:
        pairs = [(i, i ^ bit) for i in range(n)]
        held = held + [(o ^ bit, lax.ppermute(a, "shard", pairs)) for o, a in held]
        bit //= 2
    return held


def body(n, master_down, router_weight, router_gain):
    experts, inner, wide = master_down.shape
    rows = experts * inner
    scale_down = summed_scale(jnp.sum(master_down * master_down, axis=2), n)
    flat = master_down.reshape(rows, wide)
    flat_scale = scale_down.reshape(rows, 1)

    narrow = []
    for first, tall, unit in chunks(rows, inner):
        part = flat[first : first + tall] / flat_scale[first : first + tall]
        narrow.append((first, unit, part.astype(jnp.bfloat16)))
    out = None
    for first, unit, part in narrow:
        out = place(out, doubled(part, n), first, unit, rows)
    final_down = out.reshape(experts, inner, wide * n)

    part_router = (router_weight * router_gain[:, None]).astype(jnp.bfloat16).T
    held = doubled(part_router, n)
    deep = part_router.shape[1]
    me = lax.axis_index("shard")
    row_router = jnp.zeros((part_router.shape[0], deep * n), jnp.bfloat16)
    for offset, array in held:
        row_router = lax.dynamic_update_slice(
            row_router, array, (0, lax.bitwise_xor(me, offset) * deep)
        )
    serve_router = lax.all_gather(row_router, "expert", axis=0, tiled=True).T
    return (final_down, scale_down, serve_router)


def solution(mesh):
    return jax.shard_map(
        functools.partial(body, mesh.shape["shard"]),
        mesh=mesh,
        in_specs=(P("expert", None, "shard"), P("shard", "expert"), P("shard")),
        out_specs=(P("expert", None, None), P("expert", None), P()),
        check_vma=False,
    )
```

```python
import functools

import jax
import jax.numpy as jnp
from jax import lax
from jax.experimental import pallas as pl
from jax.experimental.pallas import tpu as pltpu
from jax.sharding import PartitionSpec as P


LANES = 128


def sum_kernel(n, part_ref, router_ref, scale_ref, rows_ref, slots, routers, send_sem, recv_sem):
    me = lax.axis_index("shard")
    barrier = pltpu.get_barrier_semaphore()
    for step in range(1, n):
        pl.semaphore_signal(
            barrier,
            inc=1,
            device_id={"shard": lax.rem(me + step, n)},
            device_id_type=pl.DeviceIdType.MESH,
        )
    pl.semaphore_wait(barrier, n - 1)
    copies = []
    for kind, (source, target) in enumerate(((part_ref, slots), (router_ref, routers))):
        for step in range(1, n):
            copies.append(
                pltpu.make_async_remote_copy(
                    src_ref=source,
                    dst_ref=target.at[me],
                    send_sem=send_sem.at[kind, step - 1],
                    recv_sem=recv_sem.at[kind, step - 1],
                    device_id={"shard": lax.rem(me + step, n)},
                    device_id_type=pl.DeviceIdType.MESH,
                )
            )
            copies[-1].start()
    slots[me] = part_ref[...]
    routers[me] = router_ref[...]
    for copy in copies:
        copy.wait()
    total = slots[0]
    for step in range(1, n):
        total = total + slots[step]
    scale_ref[...] = jnp.sqrt(total)
    deep = router_ref.shape[1]
    for step in range(n):
        rows_ref[:, step * deep : (step + 1) * deep] = routers[step]


def summed_scale(part, router, n):
    return pl.pallas_call(
        functools.partial(sum_kernel, n),
        out_shape=(
            jax.ShapeDtypeStruct(part.shape, jnp.float32),
            jax.ShapeDtypeStruct((router.shape[0], n * router.shape[1]), router.dtype),
        ),
        in_specs=[pl.BlockSpec(memory_space=pltpu.VMEM)] * 2,
        out_specs=(pl.BlockSpec(memory_space=pltpu.VMEM),) * 2,
        scratch_shapes=[
            pltpu.VMEM((n,) + part.shape, jnp.float32),
            pltpu.VMEM((n,) + router.shape, router.dtype),
            pltpu.SemaphoreType.DMA((2, n - 1)),
            pltpu.SemaphoreType.DMA((2, n - 1)),
        ],
        compiler_params=pltpu.CompilerParams(collective_id=0, has_side_effects=True),
        name="sum_squares",
    )(part, router)


def narrow_kernel(first, master_ref, scale_ref, out_ref):
    tall, wide = master_ref.shape
    per = scale_ref.shape[1] // tall
    block = first + pl.program_id(0)
    whole = scale_ref[pl.ds(lax.div(block, per), 1), :]
    row = whole[:, :tall]
    for at in range(1, per):
        row = jnp.where(lax.rem(block, per) == at, whole[:, at * tall : (at + 1) * tall], row)
    inverse = 1.0 / jnp.broadcast_to(row, (tall, tall)).T
    for at in range(0, wide, tall):
        out_ref[:, at : at + tall] = (master_ref[:, at : at + tall] * inverse).astype(jnp.bfloat16)


def narrowed(flat, scale, first, tall):
    wide = flat.shape[1]
    start = first // LANES
    return pl.pallas_call(
        functools.partial(narrow_kernel, start),
        grid=(tall // LANES,),
        out_shape=jax.ShapeDtypeStruct((tall, wide), jnp.bfloat16),
        in_specs=[
            pl.BlockSpec((LANES, wide), lambda i: (start + i, 0)),
            pl.BlockSpec(memory_space=pltpu.VMEM),
        ],
        out_specs=pl.BlockSpec((LANES, wide), lambda i: (i, 0)),
        cost_estimate=pl.CostEstimate(
            flops=tall * wide, bytes_accessed=6 * tall * wide, transcendentals=0
        ),
        name="narrow",
    )(flat, scale)


def place_kernel(offsets, *refs):
    me = lax.axis_index("shard")
    out_ref = refs[-1]
    for offset, ref in zip(offsets, refs):
        wide = ref.shape[1]
        at = pl.multiple_of(lax.bitwise_xor(me, jnp.int32(offset)) * wide, wide)
        out_ref[:, pl.ds(at, wide)] = ref[...]


def place(out, pieces, first, rows, carried):
    offsets = [offset for offset, _ in pieces]
    arrays = [array for _, array in pieces]
    tall, wide = arrays[0].shape
    full = wide * len(offsets)
    start = first // LANES
    anywhere = pl.BlockSpec(memory_space=pl.ANY)
    passed = list(carried) + ([] if out is None else [out])
    aliases = {len(arrays) + i: i for i in range(len(passed))}
    outs = pl.pallas_call(
        functools.partial(place_kernel, offsets),
        grid=(tall // LANES,),
        out_shape=[jax.ShapeDtypeStruct(a.shape, a.dtype) for a in carried]
        + [jax.ShapeDtypeStruct((rows, full), jnp.bfloat16)],
        in_specs=[pl.BlockSpec((LANES, wide), lambda i: (i, 0))] * len(arrays)
        + [anywhere] * len(passed),
        out_specs=[anywhere] * len(carried)
        + [pl.BlockSpec((LANES, full), lambda i: (start + i, 0))],
        input_output_aliases=aliases,
        cost_estimate=pl.CostEstimate(
            flops=tall * full, bytes_accessed=4 * tall * full, transcendentals=0
        ),
        name="place",
    )(*arrays, *passed)
    return outs[-1], list(outs[:-1])


def chunks(rows, inner):
    unit = inner // 2
    left = rows // unit
    most = max(1, left // 8)
    first, grown = 0, 1
    while left:
        take = max(1, min(most, left // 2, grown))
        yield first, take * unit
        first += take * unit
        left -= take
        grown = min(most, 3 * grown)


def step_of(held, bit, n):
    pairs = [(i, i ^ bit) for i in range(n)]
    sent = []
    for o, a in held:
        sent.append((o ^ bit, lax.ppermute(a, "shard", pairs)))
    return held + sent


def body(n, master_down, router_weight, router_gain):
    experts, inner, wide = master_down.shape
    rows = experts * inner
    part_router = (router_weight * router_gain[:, None]).astype(jnp.bfloat16).T
    scale_down, row_router = summed_scale(
        jnp.sum(master_down * master_down, axis=2), part_router, n
    )
    flat = master_down.reshape(rows, wide)

    cuts = list(chunks(rows, inner))
    near = [
        step_of([(0, narrowed(flat, scale_down, first, tall))], n // 2, n)
        for first, tall in cuts
    ]
    out, serve_router = None, None
    gathered_at = min(4, len(cuts) - 2)
    for k, (first, _) in enumerate(cuts):
        held = near[k]
        bit = n // 4
        while bit:
            held = step_of(held, bit, n)
            bit //= 2
        carried = []
        if k + 2 < len(cuts):
            carried.append(near[k + 1][1][1])
        if k == 0:
            carried.append(row_router)
        if k == gathered_at:
            carried.append(serve_router)
        out, carried = place(out, held, first, rows, carried)
        if k == 0:
            row_router = carried.pop()
            serve_router = lax.all_gather(row_router, "expert", axis=0, tiled=True).T
        if k == gathered_at:
            serve_router = carried.pop()
        if k + 2 < len(cuts):
            near[k + 1][1] = (near[k + 1][1][0], carried[0])
    return (out.reshape(experts, inner, wide * n), scale_down, serve_router)


def solution(mesh):
    n = mesh.shape["shard"]

    def step(*args):
        return body(n, *args)

    return jax.shard_map(
        step,
        mesh=mesh,
        in_specs=(P("expert", None, "shard"), P("shard", "expert"), P("shard")),
        out_specs=(P("expert", None, None), P("expert", None), P()),
        check_vma=False,
    )
```
